32 devices in a mesh: dp: 4 (over y, core), tensor: 8 (over z, x).
Axes of the slice: x: 2, y: 2, z: 4, core: 2. Of those that a mesh axis runs over, the one named last changes fastest.
Arguments:
- hidden_in: bfloat16 [512, 8192], P('dp'), may hold values from -20 to 20
- norm_gain: bfloat16 [8192], replicated, may hold values from 0.25 to 1.75
- q_weight: bfloat16 [8192, 8192], P(None, 'tensor'), as said below
- q_grad: bfloat16 [512, 8192], P('dp', 'tensor'), may hold values from -6 to 6
- q_main: float32 [8192, 8192], P('dp', 'tensor'), may hold values from -6 to 6
- weight_main_gradient: float32 [8192], P('tensor'), may hold values from -6 to 6
Outputs:
- hidden_state_gradient: bfloat16 [512, 8192], P('dp', 'tensor')
- q_main_new: float32 [8192, 8192], P('dp', 'tensor')
- weight_main_updated: float32 [8192], P('tensor')
The draws below stay inside these ranges and needn't reach their ends.
Inputs may be any that keep to these rules, and one draw needn't show every extreme that they name: `q_weight`: entries of mean 0 and deviation about 8192 ** -0.5.
All inputs are finite; a program needn't handle non-finite values.
Results may differ from the reference program's by a relative error of at most 0.03.
Values may be sent and summed in bfloat16 or wider, within the bound.
A program may use at most 128 MiB of HBM per device.

```python
import jax
import jax.numpy as jnp
from jax import lax

D = 8192
TOK_DEV = 128
TOKENS = 512
N_DP = 4
N_TENSOR = 8


def query_grads(key):
    grad_key = jax.random.fold_in(key, 11)
    values = jnp.clip(jax.random.normal(grad_key, (TOKENS, D), jnp.float32), -6.0, 6.0)
    return values.astype(jnp.bfloat16)


def query_weights(key):
    weight_key = jax.random.fold_in(key, 12)
    values = jnp.clip(jax.random.normal(weight_key, (D, D), jnp.float32), -6.0, 6.0) * D ** (-0.5)
    return values.astype(jnp.bfloat16)


def draw_q_grad(key, part):
    return query_grads(key)


def draw_q_weight(key, part):
    return query_weights(key)


def draw_hidden_in(key, part):
    grads = query_grads(key)
    weights = query_weights(key)
    direction = jnp.dot(grads, weights.T, preferred_element_type=jnp.float32)
    direction = direction * jax.lax.rsqrt(jnp.mean(direction * direction, axis=1, keepdims=True) + 1e-06)
    noise_key = jax.random.fold_in(key, 21)
    sign_key = jax.random.fold_in(key, 22)
    strength_key = jax.random.fold_in(key, 23)
    perm_key = jax.random.fold_in(key, 24)
    noise = jnp.clip(jax.random.normal(noise_key, (TOKENS, D), jnp.float32), -6.0, 6.0)
    owners = jax.random.permutation(perm_key, N_DP)
    row_block = jnp.arange(TOKENS, dtype=jnp.int32) // TOK_DEV
    col_block = jnp.arange(D, dtype=jnp.int32) // (D // N_DP)
    spike = jnp.where(owners[row_block][:, None] == col_block[None, :], 2.5, 1.0)
    signs = jnp.where(jax.random.bernoulli(sign_key, 0.5, (TOKENS, 1)), 1.0, -1.0)
    strength = jax.random.uniform(strength_key, (TOKENS, 1), jnp.float32, 0.6, 1.2)
    values = noise * spike + signs * strength * direction
    return jnp.clip(values, -20.0, 20.0).astype(jnp.bfloat16)


def level_of(stream_key, dims, shards, low, largest):
    factor_of = 1.0
    for axis_at, shards_of in shards:
        draws = jax.random.uniform(jax.random.fold_in(jax.random.fold_in(stream_key, 6), axis_at), (shards_of,), jnp.float32, low / len(shards), largest / len(shards))
        factor_of = factor_of * jnp.repeat(jnp.exp(draws), dims[axis_at] // shards_of).reshape((-1,) + (1,) * (len(dims) - 1 - axis_at))
    return factor_of


def centred(rng, dims, width, reach, split=(), kind=jnp.bfloat16):
    gain = level_of(rng, dims, split, -0.22, 0.18) if split else 1.0
    values = jax.random.normal(rng, dims, jnp.float32) * width * gain
    return jnp.minimum(jnp.maximum(values, -reach), reach).astype(kind)


def setup_inputs(seed: int = 0) -> dict:
    arg_keys = jax.random.split(jax.random.key(seed), 7)
    hidden_in = draw_hidden_in(jax.random.fold_in(arg_keys[6], 71), 0)
    norm_gain = jnp.clip(1.0 + 0.15 * jax.random.normal(arg_keys[1], (D,), jnp.float32), 0.25, 1.75).astype(jnp.bfloat16)
    q_weight = draw_q_weight(jax.random.fold_in(arg_keys[6], 71), 0)
    q_grad = draw_q_grad(jax.random.fold_in(arg_keys[6], 71), 0)
    q_main = centred(arg_keys[4], (D, D), 1.0, 6.0, ((0, 4), (1, 8)), jnp.float32)
    weight_main_gradient = centred(arg_keys[5], (D,), 1.0, 6.0, ((0, 8),), jnp.float32)
    return {"hidden_in": hidden_in, "norm_gain": norm_gain, "q_weight": q_weight, "q_grad": q_grad, "q_main": q_main, "weight_main_gradient": weight_main_gradient}


def reference(hidden_in, norm_gain, q_weight, q_grad, q_main, weight_main_gradient):
    hidden_state = hidden_in.astype(jnp.float32)
    inverse_root_mean = lax.rsqrt(lax.optimization_barrier(jnp.mean(hidden_state * hidden_state, axis=-1, keepdims=True)) + 1e-05)
    normalized_rows = hidden_state * inverse_root_mean
    norm_weight = norm_gain.astype(jnp.float32)
    normalized_input = (normalized_rows * norm_weight).astype(jnp.bfloat16)
    block = D // N_TENSOR

    def tensor_step(total, index):
        start = (index * block).astype(jnp.int32)
        grad_cols = lax.dynamic_slice_in_dim(q_grad, start, block, 1)
        weight_cols = lax.dynamic_slice_in_dim(q_weight, start, block, 1)
        term = jnp.dot(grad_cols, weight_cols.T, preferred_element_type=jnp.float32).astype(jnp.bfloat16)
        term = lax.optimization_barrier(term)
        return (total + term.astype(jnp.float32), None)
    normalized_gradient, unused = lax.scan(tensor_step, jnp.zeros((TOKENS, D), jnp.float32), jnp.arange(N_TENSOR, dtype=jnp.int32))
    scaled_gradient = normalized_gradient * norm_weight
    row_statistic = lax.optimization_barrier(jnp.mean(scaled_gradient * normalized_rows, axis=-1, keepdims=True))
    hidden_state_gradient = (inverse_root_mean * (scaled_gradient - normalized_rows * row_statistic)).astype(jnp.bfloat16)
    weight_main_updated = weight_main_gradient + lax.optimization_barrier(jnp.sum(normalized_gradient * normalized_rows, axis=0)) / N_DP

    def data_step(total, index):
        start = (index * TOK_DEV).astype(jnp.int32)
        rows = lax.dynamic_slice_in_dim(normalized_input, start, TOK_DEV, 0)
        grads = lax.dynamic_slice_in_dim(q_grad, start, TOK_DEV, 0)
        term = (jnp.dot(rows.T, grads, preferred_element_type=jnp.float32) / N_DP).astype(jnp.bfloat16)
        term = lax.optimization_barrier(term)
        return (total + term.astype(jnp.float32), None)
    q_main_new, unused_two = lax.scan(data_step, q_main, jnp.arange(N_DP, dtype=jnp.int32))
    return (hidden_state_gradient, q_main_new, weight_main_updated)
```

```python
import functools

import jax
import jax.numpy as jnp
from jax import lax
from jax.experimental import pallas as pl
from jax.experimental.pallas import tpu as pltpu
from jax.sharding import PartitionSpec as P

MESH = pl.DeviceIdType.MESH
F32 = jnp.float32
BF16 = jnp.bfloat16
NT_DIMS = (((1,), (1,)), ((), ()))


def kernel(
    ndp, nt,
    hid, gain, qg, w_hbm, wmg,
    hsg, hg, gg, wmu,
    wbuf, own, xsend, xrecv, zsend, zrecv, gs, stat_acc, ssend, srecv, wsend, wrecv,
    wsem, lsem, xs, xr, zs, zr, hs, hr, gsnd, grcv, ss, sr, ws, wr,
):
    tokens, width = hid.shape
    chunk = width // nt
    rows = width // ndp
    no, ny = nt // 2, ndp // 2
    p, t = lax.axis_index("dp"), lax.axis_index("tensor")
    y, c = p // 2, p % 2
    o, x = t // 2, t % 2
    xpeer = o * 2 + (1 - x)

    def remote(src, dst, send, recv, dev_p, dev_t):
        return pltpu.make_async_remote_copy(
            src_ref=src, dst_ref=dst, send_sem=send, recv_sem=recv,
            device_id=(dev_p, dev_t), device_id_type=MESH)

    barrier = pltpu.get_barrier_semaphore()
    for k in range(1, nt):
        pl.semaphore_signal(barrier, inc=1, device_id=(p, (t + k) % nt), device_id_type=MESH)
    for k in range(1, ndp):
        pl.semaphore_signal(barrier, inc=1, device_id=((p + k) % ndp, t), device_id_type=MESH)

    targets = [(o + s + 1) % no for s in range(no)]
    order = [targets[s] * 2 + (1 - x) for s in range(no)] + [targets[s] * 2 + x for s in range(no)]
    loads = []
    for i in range(nt):
        load = pltpu.make_async_copy(
            w_hbm.at[pl.ds(pl.multiple_of(order[i] * chunk, chunk), chunk), :], wbuf.at[i], wsem.at[i])
        load.start()
        loads.append(load)

    def peer(j):
        ky, cc = j // 2, j % 2
        return ((y + ky) % ny) * 2 + ((c + cc) % 2)

    def hid_cols(q):
        return hid.at[:, pl.ds(pl.multiple_of(q * rows, rows), rows)]

    local_h = pltpu.make_async_copy(hid_cols(p), hg.at[0], lsem.at[0])
    local_h.start()
    pl.semaphore_wait(barrier, nt - 1 + ndp - 1)

    hcopies = {}
    for j in list(range(3, ndp, 2)) + [1]:
        hcopies[j] = remote(hid_cols(peer(j)), hg.at[j], hs.at[j], hr.at[j], peer(j), t)
        hcopies[j].start()

    step_w = min(512, width)

    def square(i, total):
        v = hid[:, pl.ds(pl.multiple_of(i * step_w, step_w), step_w)].astype(F32)
        v = v * v
        for k in range(step_w // 128):
            total = total + v[:, k * 128:(k + 1) * 128]
        return total

    total = lax.fori_loop(0, width // step_w, square, jnp.zeros((tokens, 128), F32))
    rinv = lax.rsqrt(jnp.sum(total, axis=1, keepdims=True) / width + 1e-05)
    gs[...] = (qg[...].astype(F32) * rinv).astype(BF16)
    local_g = pltpu.make_async_copy(gs, gg.at[0], lsem.at[1])
    local_g.start()
    gcopies = {}
    for j in list(range(2, ndp, 2)) + [1]:
        gcopies[j] = remote(gs, gg.at[j], gsnd.at[j], grcv.at[j], peer(j), t)
        gcopies[j].start()
    for j in range(2, ndp, 2):
        hcopies[j] = remote(hid_cols(peer(j)), hg.at[j], hs.at[j], hr.at[j], peer(j), t)
        hcopies[j].start()

    stat_acc[...] = jnp.zeros_like(stat_acc)
    tile = min(256, chunk)

    def compute(i, store):
        loads[i].wait()

        @pl.loop(0, chunk // tile)
        def _(n):
            at = pl.multiple_of(n * tile, tile)
            part = lax.dot_general(
                qg[...], wbuf[i, pl.ds(at, tile), :], NT_DIMS, preferred_element_type=F32)
            store(at, part)
            cols = pl.ds(pl.multiple_of(order[i] * chunk + at, tile), tile)
            v = part * gain[:, cols].astype(F32) * hid[:, cols].astype(F32)
            for k in range(tile // 128):
                stat_acc[...] += v[:, k * 128:(k + 1) * 128]

    xcopies = []
    for s in range(no):
        def put(at, part, s=s):
            xsend[s, :, pl.ds(at, tile)] = part.astype(BF16)
        compute(s, put)
        copy = remote(xsend.at[s], xrecv.at[s], xs.at[s], xr.at[s], p, xpeer)
        copy.start()
        xcopies.append(copy)
    for s in range(no):
        def put(at, part, s=s):
            own[s, :, pl.ds(at, tile)] = part
        compute(no + s, put)

    mine = jnp.sum((stat_acc[...] * (rinv / width)).T, axis=0, keepdims=True)
    ssend[...] = jnp.broadcast_to(mine, ssend.shape)
    scopies = []
    for k in range(1, nt):
        copy = remote(ssend, srecv.at[k], ss.at[k], sr.at[k], p, (t + k) % nt)
        copy.start()
        scopies.append(copy)

    zcopies = []
    for s in range(no - 1):
        xcopies[s].wait_recv()
        zsend[s] = (own[s] + xrecv[s].astype(F32)).astype(BF16)
        copy = remote(zsend.at[s], zrecv.at[s], zs.at[s], zr.at[s], p, targets[s] * 2 + x)
        copy.start()
        zcopies.append(copy)

    rcopies = {}
    for j in range(2, ndp, 2):
        gcopies[j].wait_recv()
        rcopies[j + 1] = remote(gg.at[j], gg.at[j + 1], gsnd.at[j + 1], grcv.at[j + 1], y * 2 + (1 - c), t)
        rcopies[j + 1].start()

    xcopies[no - 1].wait_recv()
    ng = own[no - 1] + xrecv[no - 1].astype(F32)
    for s in range(no - 1):
        zcopies[s].wait_recv()
        ng = ng + zrecv[s].astype(F32)
    own[0] = ng
    mycols = pl.ds(pl.multiple_of(t * chunk, chunk), chunk)
    xhat = hid[:, mycols].astype(F32) * rinv
    contribution = jnp.sum(own[0] * xhat, axis=0, keepdims=True)
    wsend[...] = jnp.broadcast_to(contribution, wsend.shape)
    wcopies = []
    for k in range(1, ndp):
        copy = remote(wsend, wrecv.at[k], ws.at[k], wr.at[k], (p + k) % ndp, t)
        copy.start()
        wcopies.append(copy)

    stat = mine
    for k in range(1, nt):
        scopies[k - 1].wait_recv()
        stat = stat + srecv[k, 0:1, :]
    stat_col = jnp.broadcast_to(stat, (tokens, tokens)).T[:, 0:1]
    hsg[...] = (rinv * (own[0] * gain[:, mycols].astype(F32) - xhat * stat_col)).astype(BF16)

    weight = wsend[0:1, :]
    for k in range(1, ndp):
        wcopies[k - 1].wait_recv()
        weight = weight + wrecv[k, 0:1, :]
    wmu[...] = wmg[...] + weight / ndp

    for copy in rcopies.values():
        copy.wait_recv()
    gcopies[1].wait_recv()
    for copy in hcopies.values():
        copy.wait_recv()
    local_h.wait()
    local_g.wait()
    for copy in (*xcopies, *zcopies, *scopies, *wcopies, *gcopies.values(), *rcopies.values(), *hcopies.values()):
        copy.wait_send()


def body(ndp, nt, hidden_in, norm_gain, q_weight, q_grad, q_main, weight_main_gradient):
    tokens, width = hidden_in.shape
    features = q_weight.shape[1]
    chunk, rows, no = width // nt, width // ndp, nt // 2
    vmem = pl.BlockSpec(memory_space=pltpu.VMEM)
    anywhere = pl.BlockSpec(memory_space=pl.ANY)
    dma = pltpu.SemaphoreType.DMA
    hsg, hg, gg, wmu = pl.pallas_call(
        functools.partial(kernel, ndp, nt),
        out_shape=(
            jax.ShapeDtypeStruct((tokens, chunk), BF16),
            jax.ShapeDtypeStruct((ndp, tokens, rows), BF16),
            jax.ShapeDtypeStruct((ndp, tokens, features), BF16),
            jax.ShapeDtypeStruct((1, chunk), F32),
        ),
        in_specs=[vmem, vmem, vmem, anywhere, vmem],
        out_specs=(vmem, anywhere, anywhere, vmem),
        scratch_shapes=[
            pltpu.VMEM((nt, chunk, features), BF16),
            pltpu.VMEM((no, tokens, chunk), F32),
            pltpu.VMEM((no, tokens, chunk), BF16),
            pltpu.VMEM((no, tokens, chunk), BF16),
            pltpu.VMEM((no, tokens, chunk), BF16),
            pltpu.VMEM((no, tokens, chunk), BF16),
            pltpu.VMEM((tokens, features), BF16),
            pltpu.VMEM((tokens, 128), F32),
            pltpu.VMEM((8, tokens), F32),
            pltpu.VMEM((nt, 8, tokens), F32),
            pltpu.VMEM((8, chunk), F32),
            pltpu.VMEM((ndp, 8, chunk), F32),
            dma((nt,)), dma((2,)),
            dma((no,)), dma((no,)), dma((no,)), dma((no,)),
            dma((ndp,)), dma((ndp,)), dma((ndp,)), dma((ndp,)),
            dma((nt,)), dma((nt,)), dma((ndp,)), dma((ndp,)),
        ],
        compiler_params=pltpu.CompilerParams(
            collective_id=0, has_side_effects=True, vmem_limit_bytes=56 * 1024 * 1024),
    )(hidden_in, norm_gain.reshape(1, width), q_grad, q_weight, weight_main_gradient.reshape(1, chunk))
    product = lax.dot_general(
        hg.reshape(ndp * tokens, rows), gg.reshape(ndp * tokens, features),
        (((0,), (0,)), ((), ())), preferred_element_type=F32)
    gain_rows = lax.dynamic_slice_in_dim(norm_gain, lax.axis_index("dp") * rows, rows, 0)
    q_main_new = q_main + product * (gain_rows.astype(F32) / ndp)[:, None]
    return hsg, q_main_new, wmu.reshape(chunk)


def solution(mesh):
    ndp, nt = mesh.shape["dp"], mesh.shape["tensor"]
    in_specs = (
        P("dp", None),
        P(),
        P(None, "tensor"),
        P("dp", "tensor"),
        P("dp", "tensor"),
        P("tensor"),
    )
    out_specs = (P("dp", "tensor"), P("dp", "tensor"), P("tensor"))
    return jax.shard_map(
        functools.partial(body, ndp, nt), mesh=mesh, in_specs=in_specs, out_specs=out_specs, check_vma=False)
```

```python
import functools

import jax
import jax.numpy as jnp
from jax import lax
from jax.experimental import pallas as pl
from jax.experimental.pallas import tpu as pltpu
from jax.sharding import PartitionSpec as P

MESH = pl.DeviceIdType.MESH
F32 = jnp.float32
BF16 = jnp.bfloat16
NT_DIMS = (((1,), (1,)), ((), ()))


PARTS = 2
SLOTS = 8
VMEM_MIB = 28


def kernel(
    ndp, nt,
    hid_hbm, gain_in, qg, w_hbm, wmg,
    hsg, hg, gg, wmu, gout,
    hid, gain, wbuf, own, xsend, xrecv, zsend, zrecv, gs, stat_acc, ssend, srecv, wsend, wrecv,
    wsem, lsem, xs, xr, zs, zr, hs, hr, gsnd, grcv, ss, sr, ws, wr,
):
    tokens, width = hid.shape
    chunk = width // nt
    piece = chunk // PARTS
    rows = width // ndp
    no, ny = nt // 2, ndp // 2
    p, t = lax.axis_index("dp"), lax.axis_index("tensor")
    y, c = p // 2, p % 2
    o, x = t // 2, t % 2
    xpeer = o * 2 + (1 - x)

    def remote(src, dst, send, recv, dev_p, dev_t):
        copy = pltpu.make_async_remote_copy(
            src_ref=src, dst_ref=dst, send_sem=send, recv_sem=recv,
            device_id=(dev_p, dev_t), device_id_type=MESH)
        copy.start()
        return copy

    barrier = pltpu.get_barrier_semaphore()
    for k in range(1, nt):
        pl.semaphore_signal(barrier, inc=1, device_id=(p, (t + k) % nt), device_id_type=MESH)
    for k in range(1, ndp):
        pl.semaphore_signal(barrier, inc=1, device_id=((p + k) % ndp, t), device_id_type=MESH)

    def flip(k):
        value, bit = o, 1
        while bit < no:
            if k & bit:
                value = value + bit - 2 * bit * ((o // bit) % 2)
            bit *= 2
        return value

    units = [(k, h) for k in range(no - 1, -1, -1) for h in range(PARTS)]
    away = [(k, h, 1) for k, h in units]
    home = [(k, h, 0) for k, h in units]
    plan = away[:2]
    for i in range(len(units)):
        plan.append(home[i])
        if i + 2 < len(units):
            plan.append(away[i + 2])

    def column(unit):
        k, h, far = unit
        side = (1 - x) if far else x
        return pl.multiple_of((flip(k) * 2 + side) * chunk + h * piece, piece)

    loads = {}

    def load(i):
        if i < len(plan):
            loads[i] = pltpu.make_async_copy(
                w_hbm.at[pl.ds(column(plan[i]), piece), :], wbuf.at[i % SLOTS], wsem.at[i % SLOTS])
            loads[i].start()

    load(0)
    load_h = pltpu.make_async_copy(hid_hbm, hid, lsem.at[2])
    load_h.start()
    for i in range(1, 4):
        load(i)

    def peer(j):
        ky, cc = j // 2, j % 2
        return ((y + ky) % ny) * 2 + ((c + cc) % 2)

    def hid_cols(ref, q):
        return ref.at[:, pl.ds(pl.multiple_of(q * rows, rows), rows)]

    gain[...] = gain_in[...].astype(F32)
    pl.semaphore_wait(barrier, nt - 1 + ndp - 1)

    hcopies, gcopies, rcopies = {}, {}, {}

    def send_hidden(j):
        hcopies[j] = remote(hid_cols(hid_hbm, peer(j)), hg.at[j], hs.at[j], hr.at[j], peer(j), t)

    for j in range(3, ndp, 2):
        send_hidden(j)

    stat_acc[...] = jnp.zeros_like(stat_acc)
    tile = min(256, piece)
    xcopies, zcopies = {}, {}

    def compute(i):
        k, h, far = plan[i]
        loads[i].wait()
        base = column(plan[i])

        @pl.loop(0, piece // tile)
        def _(n):
            at = pl.multiple_of(n * tile, tile)
            part = lax.dot_general(
                qg[...], wbuf[i % SLOTS, pl.ds(at, tile), :], NT_DIMS, preferred_element_type=F32)
            if far:
                xsend[k, h, :, pl.ds(at, tile)] = part.astype(BF16)
            else:
                own[k, h, :, pl.ds(at, tile)] = part
            for m in range(tile // 128):
                cols = pl.ds(pl.multiple_of(base + at + m * 128, 128), 128)
                line = gain[pl.ds((base + at) // 128 + m, 1), :]
                stat_acc[...] += part[:, m * 128:(m + 1) * 128] * line * hid[:, cols].astype(F32)

        load(i + 4)
        if far:
            xcopies[k, h] = remote(xsend.at[k, h], xrecv.at[k, h], xs.at[k, h], xr.at[k, h], p, xpeer)

    def reduce(k, h):
        xcopies[k, h].wait_recv()
        total = own[k, h] + xrecv[k, h].astype(F32)
        low = k & -k if k else no
        bit = 1
        while bit < low:
            zcopies[k + bit, h].wait_recv()
            total = total + zrecv[k + bit, h].astype(F32)
            bit *= 2
        if k:
            zsend[k, h] = total.astype(BF16)
            zcopies[k, h] = remote(
                zsend.at[k, h], zrecv.at[k, h], zs.at[k, h], zr.at[k, h], p, flip(low) * 2 + x)
        else:
            own[0, h] = total

    load_h.wait()
    compute(0)
    compute(1)

    step_w = min(512, width)

    def square(i, total):
        v = hid[:, pl.ds(pl.multiple_of(i * step_w, step_w), step_w)].astype(F32)
        v = v * v
        for k in range(step_w // 128):
            total = total + v[:, k * 128:(k + 1) * 128]
        return total

    total = lax.fori_loop(0, width // step_w, square, jnp.zeros((tokens, 128), F32))
    rinv = lax.rsqrt(jnp.sum(total, axis=1, keepdims=True) / width + 1e-05)
    gs[...] = (qg[...].astype(F32) * rinv).astype(BF16)
    for j in list(range(2, ndp, 2)) + [1]:
        gcopies[j] = remote(gs, gg.at[j], gsnd.at[j], grcv.at[j], peer(j), t)
    for j in list(range(2, ndp, 2)) + [1]:
        send_hidden(j)
    local_g = pltpu.make_async_copy(gs, gg.at[0], lsem.at[1])
    local_g.start()
    local_h = pltpu.make_async_copy(hid_cols(hid, p), hg.at[0], lsem.at[0])
    local_h.start()
    gout[...] = gain[pl.ds(pl.multiple_of(p * (rows // 128), rows // 128), rows // 128), :] / ndp

    done = 0
    for i in range(2, len(plan)):
        compute(i)
        if i in (8, 12) and done < PARTS and i < len(plan) - 1:
            reduce(*units[done])
            done += 1

    mine = jnp.sum((stat_acc[...] * (rinv / width)).T, axis=0, keepdims=True)
    ssend[...] = jnp.broadcast_to(mine, ssend.shape)
    scopies = {}
    for k in range(1, nt):
        scopies[k] = remote(ssend, srecv.at[k], ss.at[k], sr.at[k], p, (t + k) % nt)

    for unit in units[done:-PARTS]:
        reduce(*unit)

    for j in range(2, ndp, 2):
        gcopies[j].wait_recv()
        rcopies[j + 1] = remote(gg.at[j], gg.at[j + 1], gsnd.at[j + 1], grcv.at[j + 1], y * 2 + (1 - c), t)

    stat = mine
    for k in range(1, nt):
        scopies[k].wait_recv()
        stat = stat + srecv[k, 0:1, :]
    stat_col = jnp.broadcast_to(stat, (tokens, tokens)).T[:, 0:1]

    for h in range(PARTS):
        reduce(0, h)
        mycols = pl.ds(pl.multiple_of(t * chunk + h * piece, piece), piece)
        xhat = hid[:, mycols].astype(F32) * rinv
        contribution = jnp.sum(own[0, h] * xhat, axis=0, keepdims=True)
        wsend[:, h * piece:(h + 1) * piece] = jnp.broadcast_to(contribution, (8, piece))
    wcopies = {}
    for k in range(1, ndp):
        wcopies[k] = remote(wsend, wrecv.at[k], ws.at[k], wr.at[k], (p + k) % ndp, t)
    for h in range(PARTS):
        for m in range(piece // 128):
            part_cols = slice(m * 128, (m + 1) * 128)
            at = t * chunk + h * piece + m * 128
            line = gain[pl.ds(at // 128, 1), :]
            xhat = hid[:, pl.ds(pl.multiple_of(at, 128), 128)].astype(F32) * rinv
            value = rinv * (own[0, h, :, part_cols] * line - xhat * stat_col)
            hsg[:, h * piece + m * 128:h * piece + (m + 1) * 128] = value.astype(BF16)

    weight = wsend[0:1, :]
    for k in range(1, ndp):
        wcopies[k].wait_recv()
        weight = weight + wrecv[k, 0:1, :]
    wmu[...] = wmg[...] + weight / ndp

    for copies in (rcopies, hcopies):
        for copy in copies.values():
            copy.wait_recv()
    gcopies[1].wait_recv()
    local_h.wait()
    local_g.wait()
    for copies in (xcopies, zcopies, scopies, wcopies, gcopies, rcopies, hcopies):
        for copy in copies.values():
            copy.wait_send()


def body(ndp, nt, hidden_in, norm_gain, q_weight, q_grad, q_main, weight_main_gradient):
    tokens, width = hidden_in.shape
    features = q_weight.shape[1]
    chunk, rows, no = width // nt, width // ndp, nt // 2
    vmem = pl.BlockSpec(memory_space=pltpu.VMEM)
    anywhere = pl.BlockSpec(memory_space=pl.ANY)
    hbm = pl.BlockSpec(memory_space=pltpu.HBM)
    dma = pltpu.SemaphoreType.DMA
    piece = chunk // PARTS
    hsg, hg, gg, wmu, gout = pl.pallas_call(
        functools.partial(kernel, ndp, nt),
        out_shape=(
            jax.ShapeDtypeStruct((tokens, chunk), BF16),
            jax.ShapeDtypeStruct((ndp, tokens, rows), BF16),
            jax.ShapeDtypeStruct((ndp, tokens, features), BF16),
            jax.ShapeDtypeStruct((1, chunk), F32),
            jax.ShapeDtypeStruct((rows // 128, 128), F32),
        ),
        in_specs=[hbm, vmem, vmem, hbm, vmem],
        out_specs=(vmem, anywhere, anywhere, vmem, vmem),
        scratch_shapes=[
            pltpu.VMEM((tokens, width), BF16),
            pltpu.VMEM((width // 128, 128), F32),
            pltpu.VMEM((SLOTS, piece, features), BF16),
            pltpu.VMEM((no, PARTS, tokens, piece), F32),
            pltpu.VMEM((no, PARTS, tokens, piece), BF16),
            pltpu.VMEM((no, PARTS, tokens, piece), BF16),
            pltpu.VMEM((no, PARTS, tokens, piece), BF16),
            pltpu.VMEM((no, PARTS, tokens, piece), BF16),
            pltpu.VMEM((tokens, features), BF16),
            pltpu.VMEM((tokens, 128), F32),
            pltpu.VMEM((8, tokens), F32),
            pltpu.VMEM((nt, 8, tokens), F32),
            pltpu.VMEM((8, chunk), F32),
            pltpu.VMEM((ndp, 8, chunk), F32),
            dma((SLOTS,)), dma((3,)),
            dma((no, PARTS)), dma((no, PARTS)), dma((no, PARTS)), dma((no, PARTS)),
            dma((ndp,)), dma((ndp,)), dma((ndp,)), dma((ndp,)),
            dma((nt,)), dma((nt,)), dma((ndp,)), dma((ndp,)),
        ],
        compiler_params=pltpu.CompilerParams(
            collective_id=0, has_side_effects=True, vmem_limit_bytes=VMEM_MIB * 1024 * 1024),
    )(hidden_in, norm_gain.reshape(width // 128, 128), q_grad, q_weight, weight_main_gradient.reshape(1, chunk))
    product = lax.dot_general(
        hg.reshape(ndp * tokens, rows), gg.reshape(ndp * tokens, features),
        (((0,), (0,)), ((), ())), preferred_element_type=F32)
    q_main_new = q_main + product * gout.reshape(rows)[:, None]
    return hsg, q_main_new, wmu.reshape(chunk)


def solution(mesh):
    ndp, nt = mesh.shape["dp"], mesh.shape["tensor"]
    in_specs = (
        P("dp", None),
        P(),
        P(None, "tensor"),
        P("dp", "tensor"),
        P("dp", "tensor"),
        P("tensor"),
    )
    out_specs = (P("dp", "tensor"), P("dp", "tensor"), P("tensor"))
    return jax.shard_map(
        functools.partial(body, ndp, nt), mesh=mesh, in_specs=in_specs, out_specs=out_specs, check_vma=False)
```

```python
import functools

import jax
import jax.numpy as jnp
from jax import lax
from jax.experimental import pallas as pl
from jax.experimental.pallas import tpu as pltpu
from jax.sharding import PartitionSpec as P

MESH = pl.DeviceIdType.MESH
F32 = jnp.float32
BF16 = jnp.bfloat16
NT_DIMS = (((1,), (1,)), ((), ()))


PARTS = 2
SLOTS = 8
VMEM_KIB = 51200


def kernel(
    ndp, nt,
    hid_hbm, gain_hbm, qg_hbm, w_hbm,
    hsg, hg, gg, wmu, gout,
    hid, gain_in, qg, gain, wbuf, own, xsend, xrecv, zsend, zrecv, gs, stat_acc, ssend, srecv, wsend, wrecv,
    wsem, lsem, xs, xr, zs, zr, hs, hr, gsnd, grcv, ss, sr, ws, wr,
):
    tokens, width = hid.shape
    chunk = width // nt
    piece = chunk // PARTS
    rows = width // ndp
    no, ny = nt // 2, ndp // 2
    p, t = lax.axis_index("dp"), lax.axis_index("tensor")
    y, c = p // 2, p % 2
    o, x = t // 2, t % 2
    xpeer = o * 2 + (1 - x)

    def remote(src, dst, send, recv, dev_p, dev_t):
        copy = pltpu.make_async_remote_copy(
            src_ref=src, dst_ref=dst, send_sem=send, recv_sem=recv,
            device_id=(dev_p, dev_t), device_id_type=MESH)
        copy.start()
        return copy

    barrier = pltpu.get_barrier_semaphore()
    for k in range(1, nt):
        pl.semaphore_signal(barrier, inc=1, device_id=(p, (t + k) % nt), device_id_type=MESH)
    for k in range(1, ndp):
        pl.semaphore_signal(barrier, inc=1, device_id=((p + k) % ndp, t), device_id_type=MESH)

    def flip(k):
        value, bit = o, 1
        while bit < no:
            if k & bit:
                value = value + bit - 2 * bit * ((o // bit) % 2)
            bit *= 2
        return value

    units = [(k, h) for k in range(no - 1, -1, -1) for h in range(PARTS)]
    away = [(k, h, 1) for k, h in units]
    home = [(k, h, 0) for k, h in units]
    plan = away[:2]
    for i in range(len(units)):
        plan.append(home[i])
        if i + 2 < len(units):
            plan.append(away[i + 2])

    def column(unit):
        k, h, far = unit
        side = (1 - x) if far else x
        return pl.multiple_of((flip(k) * 2 + side) * chunk + h * piece, piece)

    loads = {}

    def load(i):
        if i < len(plan):
            loads[i] = pltpu.make_async_copy(
                w_hbm.at[pl.ds(column(plan[i]), piece), :], wbuf.at[i % SLOTS], wsem.at[i % SLOTS])
            loads[i].start()

    load(0)
    small = []
    for i, (src, dst) in enumerate(((qg_hbm, qg), (gain_hbm, gain_in))):
        small.append(pltpu.make_async_copy(src, dst, lsem.at[3 + i]))
        small[-1].start()
    load_h = pltpu.make_async_copy(hid_hbm, hid, lsem.at[2])
    load_h.start()
    for i in range(1, 4):
        load(i)

    def peer(j):
        ky, cc = j // 2, j % 2
        return ((y + ky) % ny) * 2 + ((c + cc) % 2)

    def hid_cols(ref, q):
        return ref.at[:, pl.ds(pl.multiple_of(q * rows, rows), rows)]

    pl.semaphore_wait(barrier, nt - 1 + ndp - 1)

    hcopies, gcopies, rcopies = {}, {}, {}

    def send_hidden(j):
        hcopies[j] = remote(hid_cols(hid_hbm, peer(j)), hg.at[j], hs.at[j], hr.at[j], peer(j), t)

    for j in range(3, ndp, 2):
        send_hidden(j)

    stat_acc[...] = jnp.zeros_like(stat_acc)
    tile = min(256, piece)
    xcopies, zcopies = {}, {}

    def compute(i):
        k, h, far = plan[i]
        loads[i].wait()
        base = column(plan[i])

        @pl.loop(0, piece // tile)
        def _(n):
            at = pl.multiple_of(n * tile, tile)
            part = lax.dot_general(
                qg[...], wbuf[i % SLOTS, pl.ds(at, tile), :], NT_DIMS, preferred_element_type=F32)
            if far:
                xsend[k, h, :, pl.ds(at, tile)] = part.astype(BF16)
            else:
                own[k, h, :, pl.ds(at, tile)] = part
            for m in range(tile // 128):
                cols = pl.ds(pl.multiple_of(base + at + m * 128, 128), 128)
                line = gain[pl.ds((base + at) // 128 + m, 1), :]
                stat_acc[...] += part[:, m * 128:(m + 1) * 128] * line * hid[:, cols].astype(F32)

        load(i + 4)
        if far:
            xcopies[k, h] = remote(xsend.at[k, h], xrecv.at[k, h], xs.at[k, h], xr.at[k, h], p, xpeer)

    def reduce(k, h):
        xcopies[k, h].wait_recv()
        total = own[k, h] + xrecv[k, h].astype(F32)
        low = k & -k if k else no
        bit = 1
        while bit < low:
            zcopies[k + bit, h].wait_recv()
            total = total + zrecv[k + bit, h].astype(F32)
            bit *= 2
        if k:
            zsend[k, h] = total.astype(BF16)
            zcopies[k, h] = remote(
                zsend.at[k, h], zrecv.at[k, h], zs.at[k, h], zr.at[k, h], p, flip(low) * 2 + x)
        else:
            own[0, h] = total

    small[0].wait()
    small[1].wait()
    gain[...] = gain_in[...].astype(F32)
    load_h.wait()
    compute(0)
    compute(1)

    step_w = min(512, width)

    def square(i, total):
        v = hid[:, pl.ds(pl.multiple_of(i * step_w, step_w), step_w)].astype(F32)
        v = v * v
        for k in range(step_w // 128):
            total = total + v[:, k * 128:(k + 1) * 128]
        return total

    total = lax.fori_loop(0, width // step_w, square, jnp.zeros((tokens, 128), F32))
    rinv = lax.rsqrt(jnp.sum(total, axis=1, keepdims=True) / width + 1e-05)
    gs[...] = (qg[...].astype(F32) * rinv).astype(BF16)
    for j in list(range(2, ndp, 2)) + [1]:
        gcopies[j] = remote(gs, gg.at[j], gsnd.at[j], grcv.at[j], peer(j), t)
    for j in list(range(2, ndp, 2)) + [1]:
        send_hidden(j)
    local_g = pltpu.make_async_copy(gs, gg.at[0], lsem.at[1])
    local_g.start()
    local_h = pltpu.make_async_copy(hid_cols(hid, p), hg.at[0], lsem.at[0])
    local_h.start()
    gout[...] = gain[pl.ds(pl.multiple_of(p * (rows // 128), rows // 128), rows // 128), :] / ndp

    done = 0
    for i in range(2, len(plan)):
        compute(i)
        if i in (8, 12) and done < PARTS and i < len(plan) - 1:
            reduce(*units[done])
            done += 1

    mine = jnp.sum((stat_acc[...] * (rinv / width)).T, axis=0, keepdims=True)
    ssend[...] = jnp.broadcast_to(mine, ssend.shape)
    scopies = {}
    for k in range(1, nt):
        scopies[k] = remote(ssend, srecv.at[k], ss.at[k], sr.at[k], p, (t + k) % nt)

    for unit in units[done:-PARTS]:
        reduce(*unit)

    for j in range(2, ndp, 2):
        gcopies[j].wait_recv()
        rcopies[j + 1] = remote(gg.at[j], gg.at[j + 1], gsnd.at[j + 1], grcv.at[j + 1], y * 2 + (1 - c), t)

    stat = mine
    for k in range(1, nt):
        scopies[k].wait_recv()
        stat = stat + srecv[k, 0:1, :]
    stat_col = jnp.broadcast_to(stat, (tokens, tokens)).T[:, 0:1]

    for h in range(PARTS):
        reduce(0, h)
        mycols = pl.ds(pl.multiple_of(t * chunk + h * piece, piece), piece)
        xhat = hid[:, mycols].astype(F32) * rinv
        contribution = jnp.sum(own[0, h] * xhat, axis=0, keepdims=True)
        wsend[:, h * piece:(h + 1) * piece] = jnp.broadcast_to(contribution, (8, piece))
    wcopies = {}
    for k in range(1, ndp):
        wcopies[k] = remote(wsend, wrecv.at[k], ws.at[k], wr.at[k], (p + k) % ndp, t)
    for h in range(PARTS):
        for m in range(piece // 128):
            part_cols = slice(m * 128, (m + 1) * 128)
            at = t * chunk + h * piece + m * 128
            line = gain[pl.ds(at // 128, 1), :]
            xhat = hid[:, pl.ds(pl.multiple_of(at, 128), 128)].astype(F32) * rinv
            value = rinv * (own[0, h, :, part_cols] * line - xhat * stat_col)
            hsg[:, h * piece + m * 128:h * piece + (m + 1) * 128] = value.astype(BF16)

    weight = wsend[0:1, :]
    for k in range(1, ndp):
        wcopies[k].wait_recv()
        weight = weight + wrecv[k, 0:1, :]
    wmu[...] = weight / ndp

    for copies in (rcopies, hcopies):
        for copy in copies.values():
            copy.wait_recv()
    gcopies[1].wait_recv()
    local_h.wait()
    local_g.wait()
    for copies in (xcopies, zcopies, scopies, wcopies, gcopies, rcopies, hcopies):
        for copy in copies.values():
            copy.wait_send()


def body(ndp, nt, hidden_in, norm_gain, q_weight, q_grad, q_main, weight_main_gradient):
    tokens, width = hidden_in.shape
    features = q_weight.shape[1]
    chunk, rows, no = width // nt, width // ndp, nt // 2
    vmem = pl.BlockSpec(memory_space=pltpu.VMEM)
    anywhere = pl.BlockSpec(memory_space=pl.ANY)
    dma = pltpu.SemaphoreType.DMA
    piece = chunk // PARTS
    hsg, hg, gg, wmu, gout = pl.pallas_call(
        functools.partial(kernel, ndp, nt),
        out_shape=(
            jax.ShapeDtypeStruct((tokens, chunk), BF16),
            jax.ShapeDtypeStruct((ndp, tokens, rows), BF16),
            jax.ShapeDtypeStruct((ndp, tokens, features), BF16),
            jax.ShapeDtypeStruct((1, chunk), F32),
            jax.ShapeDtypeStruct((rows // 128, 128), F32),
        ),
        in_specs=[anywhere] * 4,
        out_specs=(vmem, anywhere, anywhere, vmem, vmem),
        scratch_shapes=[
            pltpu.VMEM((tokens, width), BF16),
            pltpu.VMEM((width // 128, 128), BF16),
            pltpu.VMEM((tokens, features), BF16),
            pltpu.VMEM((width // 128, 128), F32),
            pltpu.VMEM((SLOTS, piece, features), BF16),
            pltpu.VMEM((no, PARTS, tokens, piece), F32),
            pltpu.VMEM((no, PARTS, tokens, piece), BF16),
            pltpu.VMEM((no, PARTS, tokens, piece), BF16),
            pltpu.VMEM((no, PARTS, tokens, piece), BF16),
            pltpu.VMEM((no, PARTS, tokens, piece), BF16),
            pltpu.VMEM((tokens, features), BF16),
            pltpu.VMEM((tokens, 128), F32),
            pltpu.VMEM((8, tokens), F32),
            pltpu.VMEM((nt, 8, tokens), F32),
            pltpu.VMEM((8, chunk), F32),
            pltpu.VMEM((ndp, 8, chunk), F32),
            dma((SLOTS,)), dma((5,)),
            dma((no, PARTS)), dma((no, PARTS)), dma((no, PARTS)), dma((no, PARTS)),
            dma((ndp,)), dma((ndp,)), dma((ndp,)), dma((ndp,)),
            dma((nt,)), dma((nt,)), dma((ndp,)), dma((ndp,)),
        ],
        compiler_params=pltpu.CompilerParams(
            collective_id=0, has_side_effects=True, vmem_limit_bytes=VMEM_KIB * 1024),
    )(hidden_in, norm_gain.reshape(width // 128, 128), q_grad, q_weight)
    product = lax.dot_general(
        hg.reshape(ndp * tokens, rows), gg.reshape(ndp * tokens, features),
        (((0,), (0,)), ((), ())), preferred_element_type=F32)
    q_main_new = q_main + product * gout.reshape(rows)[:, None]
    return hsg, q_main_new, weight_main_gradient + wmu.reshape(chunk)


def solution(mesh):
    ndp, nt = mesh.shape["dp"], mesh.shape["tensor"]
    in_specs = (
        P("dp", None),
        P(),
        P(None, "tensor"),
        P("dp", "tensor"),
        P("dp", "tensor"),
        P("tensor"),
    )
    out_specs = (P("dp", "tensor"), P("dp", "tensor"), P("tensor"))
    return jax.shard_map(
        functools.partial(body, ndp, nt), mesh=mesh, in_specs=in_specs, out_specs=out_specs, check_vma=False)
```
